32 devices in a mesh: rep: 8 (over z, core), tp: 4 (over y, x).
Axes of the slice: x: 2, y: 2, z: 4, core: 2. Of those that a mesh axis runs over, the one named last changes fastest.
Arguments:
- queries: bfloat16 [64, 8192], P('rep', 'tp'), may hold values from -200 to 200
- new_keys: bfloat16 [64, 1024], P('rep', 'tp'), may hold values from -6 to 6
- new_values: bfloat16 [64, 1024], P('rep', 'tp'), may hold values from -6 to 6
- key_pool: bfloat16 [768, 128, 1024], P('rep', 'tp'), may hold values from -6 to 6
- value_pool: bfloat16 [768, 128, 1024], P('rep', 'tp'), may hold values from -6 to 6
- lengths: int32 [64], replicated, may hold values from 1 to 1536, as said below
- page_table: int32 [64, 12], P('rep'), may hold values from -1 to 95, as said below
- mig_slot: int32 [8], replicated, may hold values from 0 to 7
- mig_dst: int32 [8], replicated, may hold values from 0 to 7, as said below
Outputs:
- attended: bfloat16 [64, 8192], P('rep', 'tp')
- moved_keys: bfloat16 [96, 128, 1024], P('rep', 'tp')
- moved_values: bfloat16 [96, 128, 1024], P('rep', 'tp')
The draws below stay inside these ranges and needn't reach their ends.
Inputs may be any that keep to these rules, and one draw needn't show every extreme that they name: mig_dst[r] = (r + c) mod 8 for one offset c with 1 <= c < 8, the same for every replica. `page_table`: row q lists distinct pool pages of its replica for its first ceil(lengths[q] / 128) pages and -1 after them. `lengths`: some request has exactly 1536 cached tokens.
All inputs are finite; a program needn't handle non-finite values.
Results may differ from the reference program's by a relative error of at most 0.0065.
Values may be sent and summed in bfloat16 or wider, within the bound.
A program may use at most 64 MiB of HBM per device.

```python
import math
import jax
import jax.numpy as jnp
from jax import lax

H = 64
KVH = 8
DH = 128
PAGE = 128
PAGES_REQ = 12
REQ_REP = 8
REPLICAS = 8
REQS = 64
POOL = 96
N_REP = 8


def live_lengths(key):
    drawn = jax.random.randint(jax.random.fold_in(key, 101), (REQS,), 1, PAGES_REQ * PAGE + 1)
    return drawn.at[0].set(PAGES_REQ * PAGE).astype(jnp.int32)


def draw_lengths(key, part):
    return live_lengths(key)


def draw_page_table(key, part):
    cached = live_lengths(key)
    page_count = (cached + PAGE - 1) // PAGE
    replica_keys = jax.random.split(jax.random.fold_in(key, 202), REPLICAS)
    orders = jax.vmap(lambda subkey: jax.random.permutation(subkey, POOL))(replica_keys)
    tables = orders.reshape(REQS, PAGES_REQ).astype(jnp.int32)
    columns = jnp.arange(PAGES_REQ, dtype=jnp.int32)
    return jnp.where(columns[None, :] < page_count[:, None], tables, -1).astype(jnp.int32)


def draw_mig_dst(key, part):
    stride = jax.random.randint(jax.random.fold_in(key, 303), (), 1, REPLICAS)
    return ((jnp.arange(REPLICAS, dtype=jnp.int32) + stride) % REPLICAS).astype(jnp.int32)


def draw_queries(key, part):
    base = jnp.clip(jax.random.normal(key, (REQS, H * DH), jnp.float32), -5.0, 5.0)
    base = base * 1.5
    return base.astype(jnp.bfloat16)


def with_ends(result, key, least, top_value):
    extent = result.shape
    spot = [jax.random.randint(jax.random.fold_in(key, axis), (), 0, extent[axis]) for axis in range(len(extent))]
    result = result.at[tuple(spot)].set(least)
    longest = extent.index(max(extent))
    spot[longest] = (spot[longest] + 1) % extent[longest]
    return result.at[tuple(spot)].set(top_value)


def levels(key, shape, cuts, low, top_value):
    gain, own = 1.0, jax.random.fold_in(key, 6)
    for position, parts in cuts:
        draws = jnp.exp(jax.random.uniform(jax.random.fold_in(own, position), (parts,), jnp.float32, low / len(cuts), top_value / len(cuts)))
        gain = gain * jnp.repeat(draws, shape[position] // parts).reshape([-1 if axis == position else 1 for axis in range(len(shape))])
    return gain


def scatter_about(key, shape, spread, most, shards=(), kind=jnp.bfloat16):
    values = spread * jax.random.normal(key, shape, jnp.float32)
    if shards:
        values = values * levels(key, shape, shards, -0.22, 0.18)
    return jnp.clip(values, -most, most).astype(kind)


def setup_inputs(seed: int = 0) -> dict:
    keys = jax.random.split(jax.random.key(seed), 10)
    return {
        "queries": draw_queries(jax.random.fold_in(keys[9], 71), 0),
        "new_keys": scatter_about(keys[1], (REQS, KVH * DH), 1.5, 6.0, ((0, 8), (1, 4))),
        "new_values": scatter_about(keys[2], (REQS, KVH * DH), 1.0, 6.0, ((0, 8), (1, 4))),
        "key_pool": scatter_about(keys[3], (N_REP * POOL, PAGE, KVH * DH), 1.0, 6.0, ((0, 8), (1, 4))),
        "value_pool": scatter_about(keys[4], (N_REP * POOL, PAGE, KVH * DH), 1.0, 6.0, ((0, 8), (1, 4))),
        "lengths": draw_lengths(jax.random.fold_in(keys[9], 71), 0),
        "page_table": draw_page_table(jax.random.fold_in(keys[9], 71), 0),
        "mig_slot": with_ends(jax.random.randint(keys[7], (REPLICAS,), 0, REQ_REP), jax.random.fold_in(keys[7], 1), 0, REQ_REP - 1).astype(jnp.int32),
        "mig_dst": draw_mig_dst(jax.random.fold_in(keys[9], 71), 0),
    }


def reference(queries, new_keys, new_values, key_pool, value_pool, lengths, page_table, mig_slot, mig_dst):
    replica_ids = jnp.arange(N_REP, dtype=jnp.int32)
    scaling = 1.0 / math.sqrt(DH)

    def one_replica(replica):
        source = jnp.sum(jnp.where(mig_dst == replica, replica_ids, 0)).astype(jnp.int32)
        leaving = mig_slot[replica]
        arriving = (source * REQ_REP + mig_slot[source]).astype(jnp.int32)
        slot_ids = jnp.arange(REQ_REP, dtype=jnp.int32)
        owner_rep = jnp.where(slot_ids == leaving, source, replica).astype(jnp.int32)
        owner_req = jnp.where(slot_ids == leaving, arriving, replica * REQ_REP + slot_ids).astype(jnp.int32)
        table_rows = page_table[owner_req]
        page_index = (owner_rep[:, None] * POOL + jnp.maximum(table_rows, 0)).astype(jnp.int32)
        cached_keys = key_pool[page_index].reshape(REQ_REP, PAGES_REQ * PAGE, KVH, DH).astype(jnp.float32)
        cached_values = value_pool[page_index].reshape(REQ_REP, PAGES_REQ * PAGE, KVH, DH).astype(jnp.float32)
        live_len = lengths[owner_req]
        positions = jnp.arange(PAGES_REQ * PAGE, dtype=jnp.int32)
        usable = positions[None, :] < live_len[:, None]
        start = (replica * REQ_REP).astype(jnp.int32)
        query_rows = lax.dynamic_slice_in_dim(queries, start, REQ_REP, 0).reshape(REQ_REP, KVH, H // KVH, DH).astype(jnp.float32)
        fresh_keys = lax.dynamic_slice_in_dim(new_keys, start, REQ_REP, 0).reshape(REQ_REP, KVH, DH).astype(jnp.float32)
        fresh_values = lax.dynamic_slice_in_dim(new_values, start, REQ_REP, 0).reshape(REQ_REP, KVH, DH).astype(jnp.float32)
        scores = jnp.einsum('rgqd,rngd->rgqn', query_rows, cached_keys) * scaling
        new_score = jnp.einsum('rgqd,rgd->rgq', query_rows, fresh_keys) * scaling
        masked = jnp.where(usable[:, None, None, :], scores, -jnp.inf)
        maxima = jnp.maximum(masked.max(-1), new_score)
        weights = jnp.where(usable[:, None, None, :], jnp.exp(masked - maxima[..., None]), 0.0)
        new_weight = jnp.exp(new_score - maxima)
        totals = weights.sum(-1) + new_weight
        rounded = lax.optimization_barrier(weights.astype(jnp.bfloat16)).astype(jnp.float32)
        rounded_new = lax.optimization_barrier(new_weight.astype(jnp.bfloat16)).astype(jnp.float32)
        mixed = jnp.einsum('rgqn,rngd->rgqd', rounded, cached_values)
        mixed = mixed + rounded_new[..., None] * fresh_values[:, :, None, :]
        attended = (mixed / totals[..., None]).reshape(REQ_REP, H * DH).astype(jnp.bfloat16)
        moved_rows = page_table[arriving]
        moved_index = (source * POOL + jnp.maximum(moved_rows, 0)).astype(jnp.int32)
        present = (moved_rows >= 0)[:, None, None]
        moved_keys = jnp.where(present, key_pool[moved_index], jnp.zeros((), jnp.bfloat16))
        moved_values = jnp.where(present, value_pool[moved_index], jnp.zeros((), jnp.bfloat16))
        return (attended, moved_keys, moved_values)
    attended, moved_keys, moved_values = lax.map(one_replica, replica_ids)
    return (attended.reshape(N_REP * REQ_REP, H * DH), moved_keys.reshape(N_REP * PAGES_REQ, PAGE, KVH * DH), moved_values.reshape(N_REP * PAGES_REQ, PAGE, KVH * DH))
```

```python
import math

import jax
import jax.numpy as jnp
from jax import lax
from jax.experimental import pallas as pl
from jax.experimental.pallas import tpu as pltpu
from jax.sharding import PartitionSpec as P

H = 64
KVH = 8
DH = 128
LOW = -1e30


def route_by(count, distance):
    return [(i, (i + distance) % count) for i in range(count)]


def pick_kernel(rows_ref, pool_ref, out_ref, sem):
    pages = out_ref.shape[0]

    @pl.loop(0, pages)
    def _(j):
        page = jnp.maximum(rows_ref[j], 0)
        pltpu.make_async_copy(pool_ref.at[page], out_ref.at[j], sem).start()

    pltpu.make_async_copy(pool_ref.at[pl.ds(0, pages)], out_ref, sem).wait()

    @pl.loop(0, pages)
    def _(j):
        @pl.when(rows_ref[j] < 0)
        def _():
            out_ref[j] = jnp.zeros(out_ref.shape[1:], out_ref.dtype)


def picked_pages(rows, pool):
    shape = (rows.shape[0],) + pool.shape[1:]
    size = math.prod(shape) * 2
    return pl.pallas_call(
        pick_kernel,
        out_shape=jax.ShapeDtypeStruct(shape, pool.dtype),
        in_specs=[
            pl.BlockSpec(memory_space=pltpu.SMEM),
            pl.BlockSpec(memory_space=pl.ANY),
        ],
        out_specs=pl.BlockSpec(memory_space=pltpu.VMEM),
        scratch_shapes=[pltpu.SemaphoreType.DMA],
        cost_estimate=pl.CostEstimate(flops=0, bytes_accessed=2 * size, transcendentals=0),
    )(rows, pool)


def flat_rows(block):
    pages, rows, width = block.shape
    if rows % 16 == 0:
        return block.reshape(pages * rows, width)
    return block.astype(jnp.float32).reshape(pages * rows, width).astype(block.dtype)


def attend_kernel(
    table_ref, len_ref, start_ref, q_ref, key_ref, value_ref, out_ref, kbuf, vbuf, ksem, vsem
):
    slots, pages, rows, width = kbuf.shape
    parts, _, heads_here, _ = out_ref.shape
    group = H // KVH
    tokens = pages * rows
    page_len = rows * parts
    scaling = 1.0 / math.sqrt(DH)

    @pl.loop(0, slots)
    def _(i):
        @pl.loop(0, pages)
        def _(j):
            page = jnp.maximum(table_ref[i, j], 0)
            pltpu.make_async_copy(key_ref.at[page], kbuf.at[i, j], ksem.at[i]).start()
            pltpu.make_async_copy(value_ref.at[page], vbuf.at[i, j], vsem.at[i]).start()

    lane = lax.broadcasted_iota(jnp.int32, (H, tokens), 1)
    position = (lane // rows) * page_len + lane % rows + start_ref[0]
    head = lax.broadcasted_iota(jnp.int32, (H, DH), 0) // group
    half = lax.broadcasted_iota(jnp.int32, (H, DH), 1) < DH // 2

    @pl.loop(0, slots)
    def _(i):
        q = q_ref[i].astype(jnp.float32)
        spread = jnp.concatenate(
            [jnp.where(head == g, q, 0.0).astype(jnp.bfloat16) for g in range(KVH)], axis=1
        )
        pltpu.make_async_copy(key_ref.at[pl.ds(0, pages)], kbuf.at[i], ksem.at[i]).wait()
        scores = lax.dot_general(
            spread,
            flat_rows(kbuf[i]),
            (((1,), (1,)), ((), ())),
            preferred_element_type=jnp.float32,
        )
        usable = position < len_ref[i]
        masked = jnp.where(usable, scores * scaling, LOW)
        peak = jnp.max(masked, axis=1, keepdims=True)
        weights = jnp.where(usable, jnp.exp(masked - peak), 0.0)
        total = jnp.sum(weights, axis=1, keepdims=True)
        pltpu.make_async_copy(value_ref.at[pl.ds(0, pages)], vbuf.at[i], vsem.at[i]).wait()
        mixed = jnp.dot(
            weights.astype(jnp.bfloat16), flat_rows(vbuf[i]), preferred_element_type=jnp.float32
        )
        own = jnp.concatenate(
            [
                mixed[g * group : (g + 1) * group, g * DH : (g + 1) * DH]
                for g in range(KVH)
            ],
            axis=0,
        )
        stats = jnp.where(half, peak, total)
        for t in range(parts):
            span = slice(t * heads_here, (t + 1) * heads_here)
            out_ref[t, i, :, 0:DH] = own[span]
            out_ref[t, i, :, DH : 2 * DH] = stats[span]


def attended_parts(table, lens, start, q, key_pool, value_pool, parts):
    slots, pages = table.shape
    rows, width = key_pool.shape[1:]
    buffer = (slots, pages, rows, width)
    return pl.pallas_call(
        attend_kernel,
        out_shape=jax.ShapeDtypeStruct((parts, slots, H // parts, 2 * DH), jnp.float32),
        in_specs=[pl.BlockSpec(memory_space=pltpu.SMEM)] * 3
        + [pl.BlockSpec(memory_space=pltpu.VMEM)]
        + [pl.BlockSpec(memory_space=pl.ANY)] * 2,
        out_specs=pl.BlockSpec(memory_space=pltpu.VMEM),
        scratch_shapes=[
            pltpu.VMEM(buffer, key_pool.dtype),
            pltpu.VMEM(buffer, value_pool.dtype),
            pltpu.SemaphoreType.DMA((slots,)),
            pltpu.SemaphoreType.DMA((slots,)),
        ],
        cost_estimate=pl.CostEstimate(
            flops=4 * H * pages * rows * width * slots,
            bytes_accessed=4 * math.prod(buffer),
            transcendentals=0,
        ),
    )(table, lens, start, q, key_pool, value_pool)


def finish_kernel(part_ref, q_ref, tk_ref, tv_ref, out_ref):
    parts = part_ref.shape[0]
    scaling = 1.0 / math.sqrt(DH)
    q = q_ref[...].astype(jnp.float32)
    fresh = jnp.sum(q * tk_ref[...].astype(jnp.float32), axis=-1, keepdims=True) * scaling
    peaks = [part_ref[t, :, :, DH : DH + 1] for t in range(parts)]
    top = fresh
    for t in range(parts):
        top = jnp.maximum(top, peaks[t])
    weight = jnp.exp(fresh - top)
    total = weight
    mixed = weight.astype(jnp.bfloat16).astype(jnp.float32) * tv_ref[...].astype(jnp.float32)
    for t in range(parts):
        scale = jnp.exp(peaks[t] - top)
        total = total + scale * part_ref[t, :, :, DH + DH // 2 : DH + DH // 2 + 1]
        mixed = mixed + scale * part_ref[t, :, :, 0:DH]
    out_ref[...] = (mixed / total).astype(out_ref.dtype)


def finished(partials, q, token_keys, token_values):
    return pl.pallas_call(
        finish_kernel,
        out_shape=jax.ShapeDtypeStruct(q.shape, jnp.bfloat16),
        in_specs=[pl.BlockSpec(memory_space=pltpu.VMEM)] * 4,
        out_specs=pl.BlockSpec(memory_space=pltpu.VMEM),
        cost_estimate=pl.CostEstimate(
            flops=4 * partials.size, bytes_accessed=4 * partials.size, transcendentals=0
        ),
    )(partials, q, token_keys, token_values)


def token_rows(fresh, parts, part_index):
    slots, width = fresh.shape
    heads_here = H // parts
    if width % DH == 0:
        per_head = fresh.reshape(slots, width // DH, DH)
        return jnp.repeat(per_head, heads_here * DH // width, axis=1)
    every = lax.all_gather(fresh, "tp", axis=1, tiled=True).reshape(slots, KVH, DH)
    every = jnp.repeat(every, H // KVH, axis=1)
    return lax.dynamic_slice_in_dim(every, part_index * heads_here, heads_here, 1)


def body(
    queries, new_keys, new_values, key_pool, value_pool, lengths, page_table, mig_slot, mig_dst
):
    replicas = lax.axis_size("rep")
    parts = lax.axis_size("tp")
    here_rep = lax.axis_index("rep")
    part_index = lax.axis_index("tp")
    slots, q_width = queries.shape
    k_width = new_keys.shape[1]
    heads_here = H // parts
    offset = mig_dst[0]
    leaving = mig_slot[here_rep]
    out_rows = lax.dynamic_index_in_dim(page_table, leaving, 0, keepdims=False)
    own_len = lax.dynamic_slice_in_dim(lengths, here_rep * slots, slots)
    start = (part_index * key_pool.shape[1]).reshape(1)
    is_leaving = (jnp.arange(slots) == leaving)[:, None]
    tokens = jnp.concatenate([queries, new_keys, new_values], axis=1)
    visitor = lax.dynamic_slice_in_dim(tokens, leaving, 1, 0)
    keys_out = picked_pages(out_rows, key_pool)

    def branch(distance):
        def run(tokens, visitor, keys_out):
            back = lax.ppermute(visitor, "rep", route_by(replicas, -distance))
            moved_keys = lax.ppermute(keys_out, "rep", route_by(replicas, distance))
            values_out = picked_pages(out_rows, value_pool)
            moved_values = lax.ppermute(values_out, "rep", route_by(replicas, distance))
            mine = jnp.where(is_leaving, back, tokens)
            q_own = mine[:, :q_width].reshape(slots, heads_here, DH)
            q_full = lax.all_gather(q_own, "tp", axis=1, tiled=True)
            token_keys = token_rows(mine[:, q_width : q_width + k_width], parts, part_index)
            token_values = token_rows(mine[:, q_width + k_width :], parts, part_index)
            partials = attended_parts(
                page_table, own_len, start, q_full, key_pool, value_pool, parts
            )
            partials = lax.all_to_all(partials, "tp", 0, 0, tiled=True)
            result = finished(partials, q_own, token_keys, token_values)
            result = result.reshape(slots, q_width)
            leaver = lax.dynamic_slice_in_dim(result, leaving, 1, 0)
            arrived = lax.ppermute(leaver, "rep", route_by(replicas, distance))
            attended = jnp.where(is_leaving, arrived, result)
            return attended, moved_keys, moved_values

        return run

    return lax.switch(
        offset - 1,
        [branch(distance) for distance in range(1, replicas)],
        tokens,
        visitor,
        keys_out,
    )


def solution(mesh):
    placed = (
        P("rep", "tp"),
        P("rep", "tp"),
        P("rep", "tp"),
        P("rep", "tp", None),
        P("rep", "tp", None),
        P(),
        P("rep", None),
        P(),
        P(),
    )
    return jax.shard_map(
        body,
        mesh=mesh,
        in_specs=placed,
        out_specs=(P("rep", "tp"), P("rep", "tp", None), P("rep", "tp", None)),
        check_vma=False,
    )
```

```python
import math

import jax
import jax.numpy as jnp
from jax import lax
from jax.experimental import pallas as pl
from jax.experimental.pallas import tpu as pltpu
from jax.sharding import PartitionSpec as P

H = 64
KVH = 8
DH = 128
LOW = -1e30


def route_by(count, distance):
    return [(i, (i + distance) % count) for i in range(count)]


def pick_kernel(
    table_ref, mig_ref, q_ref, nk_ref, nv_ref, key_ref, value_ref, row_ref, kout_ref, vout_ref, sems
):
    pages = kout_ref.shape[0]
    leaving = mig_ref[lax.axis_index("rep")]

    @pl.loop(0, pages)
    def _(j):
        page = jnp.maximum(table_ref[leaving, j], 0)
        pltpu.make_async_copy(key_ref.at[page], kout_ref.at[j], sems.at[0]).start()
        pltpu.make_async_copy(value_ref.at[page], vout_ref.at[j], sems.at[1]).start()

    at = 0
    for ref in (q_ref, nk_ref, nv_ref):
        width = ref.shape[1]
        slot = lax.broadcasted_iota(jnp.int32, ref.shape, 0)
        chosen = jnp.where(slot == leaving, ref[...].astype(jnp.float32), 0.0)
        row = jnp.sum(chosen, axis=0, keepdims=True)
        row_ref[:, at : at + width] = row.astype(jnp.bfloat16)
        at += width
    pltpu.make_async_copy(key_ref.at[pl.ds(0, pages)], kout_ref, sems.at[0]).wait()
    pltpu.make_async_copy(value_ref.at[pl.ds(0, pages)], vout_ref, sems.at[1]).wait()

    @pl.loop(0, pages)
    def _(j):
        @pl.when(table_ref[leaving, j] < 0)
        def _():
            kout_ref[j] = jnp.zeros(kout_ref.shape[1:], kout_ref.dtype)
            vout_ref[j] = jnp.zeros(vout_ref.shape[1:], vout_ref.dtype)


def picked(table, mig_slot, queries, new_keys, new_values, key_pool, value_pool):
    shape = (table.shape[1],) + key_pool.shape[1:]
    width = queries.shape[1] + 2 * new_keys.shape[1]
    return pl.pallas_call(
        pick_kernel,
        out_shape=[
            jax.ShapeDtypeStruct((1, width), jnp.bfloat16),
            jax.ShapeDtypeStruct(shape, key_pool.dtype),
            jax.ShapeDtypeStruct(shape, key_pool.dtype),
        ],
        in_specs=[pl.BlockSpec(memory_space=pltpu.SMEM)] * 2
        + [pl.BlockSpec(memory_space=pltpu.VMEM)] * 3
        + [pl.BlockSpec(memory_space=pl.ANY)] * 2,
        out_specs=[pl.BlockSpec(memory_space=pltpu.VMEM)] * 3,
        scratch_shapes=[pltpu.SemaphoreType.DMA((2,))],
        compiler_params=pltpu.CompilerParams(vmem_limit_bytes=8 << 20),
        cost_estimate=pl.CostEstimate(
            flops=0, bytes_accessed=8 * math.prod(shape), transcendentals=0
        ),
    )(table, mig_slot, queries, new_keys, new_values, key_pool, value_pool)


def greet(parts):
    me = lax.axis_index("tp")
    barrier = pltpu.get_barrier_semaphore()
    for k in range(1, parts):
        pl.semaphore_signal(
            barrier,
            inc=1,
            device_id={"tp": lax.rem(me + k, parts)},
            device_id_type=pl.DeviceIdType.MESH,
        )
    pl.semaphore_wait(barrier, parts - 1)
    return me


def share_kernel(mig_ref, back_ref, tokens_ref, all_ref, mine_ref, own, send_sems, recv_sems):
    parts, slots, heads_here, _ = all_ref.shape
    chunks = tokens_ref.shape[1]
    leaving = mig_ref[lax.axis_index("rep")]
    back = back_ref[...].astype(jnp.float32)
    row = jnp.concatenate([back[:, h * DH : (h + 1) * DH] for h in range(chunks)], axis=0)
    for i in range(slots):
        value = jnp.where(leaving == i, row, tokens_ref[i].astype(jnp.float32))
        value = value.astype(jnp.bfloat16)
        mine_ref[i] = value
        own[i] = value[:heads_here]
    me = greet(parts)
    copies = []
    for k in range(1, parts):
        copy = pltpu.make_async_remote_copy(
            src_ref=own,
            dst_ref=all_ref.at[me],
            send_sem=send_sems.at[k - 1],
            recv_sem=recv_sems.at[k - 1],
            device_id={"tp": lax.rem(me + k, parts)},
            device_id_type=pl.DeviceIdType.MESH,
        )
        copy.start()
        copies.append(copy)
    all_ref[me] = own[...]
    for copy in copies:
        copy.wait()


def shared(mig_slot, back, tokens, heads_here, parts):
    slots = tokens.shape[0]
    return pl.pallas_call(
        share_kernel,
        out_shape=[
            jax.ShapeDtypeStruct((parts, slots, heads_here, DH), jnp.bfloat16),
            jax.ShapeDtypeStruct(tokens.shape, jnp.bfloat16),
        ],
        in_specs=[pl.BlockSpec(memory_space=pltpu.SMEM)]
        + [pl.BlockSpec(memory_space=pltpu.VMEM)] * 2,
        out_specs=[pl.BlockSpec(memory_space=pltpu.VMEM)] * 2,
        scratch_shapes=[
            pltpu.VMEM((slots, heads_here, DH), jnp.bfloat16),
            pltpu.SemaphoreType.DMA((parts - 1,)),
            pltpu.SemaphoreType.DMA((parts - 1,)),
        ],
        compiler_params=pltpu.CompilerParams(
            collective_id=0, has_side_effects=True, vmem_limit_bytes=8 << 20
        ),
        cost_estimate=pl.CostEstimate(flops=0, bytes_accessed=8 << 20, transcendentals=0),
    )(mig_slot, back, tokens)


def flat_rows(block):
    pages, rows, width = block.shape
    if rows % 16 == 0:
        return block.reshape(pages * rows, width)
    return block.astype(jnp.float32).reshape(pages * rows, width).astype(block.dtype)


def attend_kernel(
    table_ref, len_ref, start_ref, q_ref, key_ref, value_ref, out_ref, kbuf, vbuf, ksem, vsem
):
    slots, pages, rows, width = kbuf.shape
    parts, heads_here = q_ref.shape[0], q_ref.shape[2]
    group = H // KVH
    tokens = pages * rows
    page_len = rows * parts
    scaling = 1.0 / math.sqrt(DH)

    @pl.loop(0, slots)
    def _(i):
        @pl.loop(0, pages)
        def _(j):
            page = jnp.maximum(table_ref[i, j], 0)
            pltpu.make_async_copy(key_ref.at[page], kbuf.at[i, j], ksem.at[i]).start()
            pltpu.make_async_copy(value_ref.at[page], vbuf.at[i, j], vsem.at[i]).start()

    lane = lax.broadcasted_iota(jnp.int32, (H, tokens), 1)
    position = (lane // rows) * page_len + lane % rows + start_ref[0]
    head = lax.broadcasted_iota(jnp.int32, (H, DH), 0) // group
    column = lax.broadcasted_iota(jnp.int32, (H, DH), 1)

    def turn(i, stats):
        q = jnp.concatenate([q_ref[t, i].astype(jnp.float32) for t in range(parts)], axis=0)
        spread = jnp.concatenate(
            [jnp.where(head == g, q, 0.0).astype(jnp.bfloat16) for g in range(KVH)], axis=1
        )
        pltpu.make_async_copy(key_ref.at[pl.ds(0, pages)], kbuf.at[i], ksem.at[i]).wait()
        scores = lax.dot_general(
            spread,
            flat_rows(kbuf[i]),
            (((1,), (1,)), ((), ())),
            preferred_element_type=jnp.float32,
        )
        usable = position < len_ref[i]
        masked = jnp.where(usable, scores * scaling, LOW)
        peak = jnp.max(masked, axis=1, keepdims=True)
        weights = jnp.where(usable, jnp.exp(masked - peak), 0.0)
        total = jnp.sum(weights, axis=1, keepdims=True)
        pltpu.make_async_copy(value_ref.at[pl.ds(0, pages)], vbuf.at[i], vsem.at[i]).wait()
        mixed = jnp.dot(
            weights.astype(jnp.bfloat16), flat_rows(vbuf[i]), preferred_element_type=jnp.float32
        )
        own = jnp.concatenate(
            [
                mixed[g * group : (g + 1) * group, g * DH : (g + 1) * DH]
                for g in range(KVH)
            ],
            axis=0,
        )
        for t in range(parts):
            out_ref[t, i] = own[t * heads_here : (t + 1) * heads_here]
        stats = jnp.where(column == i, peak, stats)
        return jnp.where(column == i + slots, total, stats)

    stats = lax.fori_loop(0, slots, turn, jnp.zeros((H, DH), jnp.float32))
    for t in range(parts):
        out_ref[t, slots] = stats[t * heads_here : (t + 1) * heads_here]


def attended_parts(table, lens, start, q, key_pool, value_pool, parts):
    slots, pages = table.shape
    rows, width = key_pool.shape[1:]
    buffer = (slots, pages, rows, width)
    return pl.pallas_call(
        attend_kernel,
        out_shape=jax.ShapeDtypeStruct((parts, slots + 1, H // parts, DH), jnp.float32),
        in_specs=[pl.BlockSpec(memory_space=pltpu.SMEM)] * 3
        + [pl.BlockSpec(memory_space=pltpu.VMEM)]
        + [pl.BlockSpec(memory_space=pl.ANY)] * 2,
        out_specs=pl.BlockSpec(memory_space=pltpu.VMEM),
        scratch_shapes=[
            pltpu.VMEM(buffer, key_pool.dtype),
            pltpu.VMEM(buffer, value_pool.dtype),
            pltpu.SemaphoreType.DMA((slots,)),
            pltpu.SemaphoreType.DMA((slots,)),
        ],
        compiler_params=pltpu.CompilerParams(vmem_limit_bytes=24 << 20),
        cost_estimate=pl.CostEstimate(
            flops=4 * H * pages * rows * width * slots,
            bytes_accessed=4 * math.prod(buffer),
            transcendentals=0,
        ),
    )(table, lens, start, q, key_pool, value_pool)


def finish_kernel(
    mig_ref,
    part_ref,
    mine_ref,
    tk_ref,
    tv_ref,
    out_ref,
    leaver_ref,
    flat,
    landed,
    send_sems,
    recv_sems,
):
    parts, _, heads_here, _ = part_ref.shape
    slots = mine_ref.shape[0]
    repeat = heads_here // tk_ref.shape[1]
    leaving = mig_ref[lax.axis_index("rep")]
    scaling = 1.0 / math.sqrt(DH)
    me = greet(parts)
    copies = []
    for k in range(1, parts):
        peer = lax.rem(me + k, parts)
        copy = pltpu.make_async_remote_copy(
            src_ref=part_ref.at[peer],
            dst_ref=landed.at[k - 1],
            send_sem=send_sems.at[k - 1],
            recv_sem=recv_sems.at[k - 1],
            device_id={"tp": peer},
            device_id_type=pl.DeviceIdType.MESH,
        )
        copy.start()
        copies.append(copy)

    def spread(ref, i):
        value = ref[i].astype(jnp.float32)
        return jnp.concatenate(
            [
                jnp.broadcast_to(value[g : g + 1], (repeat, DH))
                for g in range(value.shape[0])
            ],
            axis=0,
        )

    fresh, values = [], []
    for i in range(slots):
        q = mine_ref[i].astype(jnp.float32)[:heads_here]
        fresh.append(jnp.sum(q * spread(tk_ref, i), axis=-1, keepdims=True) * scaling)
        values.append(spread(tv_ref, i))
    for copy in copies:
        copy.wait()
    stats = [part_ref[me, slots]] + [landed[k, slots] for k in range(parts - 1)]
    leaver = jnp.zeros((heads_here, DH), jnp.float32)
    for i in range(slots):
        top = fresh[i]
        for stat in stats:
            top = jnp.maximum(top, stat[:, i : i + 1])
        weight = jnp.exp(fresh[i] - top)
        total = weight
        mixed = weight.astype(jnp.bfloat16).astype(jnp.float32) * values[i]
        for k, stat in enumerate(stats):
            scale = jnp.exp(stat[:, i : i + 1] - top)
            block = part_ref[me, i] if k == 0 else landed[k - 1, i]
            total = total + scale * stat[:, slots + i : slots + i + 1]
            mixed = mixed + scale * block
        result = mixed / total
        leaver = jnp.where(leaving == i, result, leaver)
        for h in range(heads_here):
            flat[i : i + 1, h * DH : (h + 1) * DH] = result[h : h + 1]
    out_ref[...] = flat[...].astype(out_ref.dtype)
    row = jnp.concatenate([leaver[h : h + 1] for h in range(heads_here)], axis=1)
    leaver_ref[...] = row.astype(leaver_ref.dtype)


def finished(mig_slot, partials, mine, token_keys, token_values):
    parts, _, heads_here, _ = partials.shape
    slots = mine.shape[0]
    return pl.pallas_call(
        finish_kernel,
        out_shape=[
            jax.ShapeDtypeStruct((slots, heads_here * DH), jnp.bfloat16),
            jax.ShapeDtypeStruct((1, heads_here * DH), jnp.bfloat16),
        ],
        in_specs=[pl.BlockSpec(memory_space=pltpu.SMEM)]
        + [pl.BlockSpec(memory_space=pltpu.VMEM)] * 4,
        out_specs=[pl.BlockSpec(memory_space=pltpu.VMEM)] * 2,
        scratch_shapes=[
            pltpu.VMEM((slots, heads_here * DH), jnp.float32),
            pltpu.VMEM((parts - 1,) + partials.shape[1:], jnp.float32),
            pltpu.SemaphoreType.DMA((parts - 1,)),
            pltpu.SemaphoreType.DMA((parts - 1,)),
        ],
        compiler_params=pltpu.CompilerParams(
            collective_id=1, has_side_effects=True, vmem_limit_bytes=8 << 20
        ),
        cost_estimate=pl.CostEstimate(flops=0, bytes_accessed=8 << 20, transcendentals=0),
    )(mig_slot, partials, mine, token_keys, token_values)


def place_kernel(
    mig_ref, result_ref, row_ref, key_ref, value_ref, out_ref, kout_ref, vout_ref, kbuf, vbuf, sems
):
    pages = kbuf.shape[0]
    lanes = ((key_ref, kbuf, kout_ref), (value_ref, vbuf, vout_ref))
    span = 3 if pages % 3 == 0 else 1
    cuts = [pl.ds(j, span) for j in range(0, pages, span)]
    pairs = [(n, c) for c in range(len(cuts)) for n in range(2)]
    for n, c in pairs:
        source, buf, _ = lanes[n]
        pltpu.make_async_copy(source.at[cuts[c]], buf.at[cuts[c]], sems.at[n, c]).start()
    leaving = mig_ref[lax.axis_index("rep")]
    slot = lax.broadcasted_iota(jnp.int32, result_ref.shape, 0)
    row = row_ref[...].astype(jnp.float32)
    result = result_ref[...].astype(jnp.float32)
    out_ref[...] = jnp.where(slot == leaving, row, result).astype(out_ref.dtype)
    for n, c in pairs:
        source, buf, sink = lanes[n]
        pltpu.make_async_copy(source.at[cuts[c]], buf.at[cuts[c]], sems.at[n, c]).wait()
        pltpu.make_async_copy(buf.at[cuts[c]], sink.at[cuts[c]], sems.at[n, c]).start()
    for n, c in pairs:
        _, buf, sink = lanes[n]
        pltpu.make_async_copy(buf.at[cuts[c]], sink.at[cuts[c]], sems.at[n, c]).wait()


def placed_results(mig_slot, result, row, moved_keys, moved_values):
    moved = jax.ShapeDtypeStruct(moved_keys.shape, moved_keys.dtype)
    return pl.pallas_call(
        place_kernel,
        out_shape=[jax.ShapeDtypeStruct(result.shape, result.dtype), moved, moved],
        in_specs=[pl.BlockSpec(memory_space=pltpu.SMEM)]
        + [pl.BlockSpec(memory_space=pltpu.VMEM)] * 2
        + [pl.BlockSpec(memory_space=pl.ANY)] * 2,
        out_specs=[pl.BlockSpec(memory_space=pltpu.VMEM)]
        + [pl.BlockSpec(memory_space=pl.ANY)] * 2,
        scratch_shapes=[
            pltpu.VMEM(moved.shape, moved.dtype),
            pltpu.VMEM(moved.shape, moved.dtype),
            pltpu.SemaphoreType.DMA((2, moved.shape[0])),
        ],
        compiler_params=pltpu.CompilerParams(vmem_limit_bytes=8 << 20),
    )(mig_slot, result, row, moved_keys, moved_values)


def token_rows(fresh, parts, part_index):
    slots, width = fresh.shape
    heads_here = H // parts
    if width % DH == 0:
        return fresh.reshape(slots, width // DH, DH)
    every = lax.all_gather(fresh, "tp", axis=1, tiled=True).reshape(slots, KVH, DH)
    every = jnp.repeat(every, H // KVH, axis=1)
    return lax.dynamic_slice_in_dim(every, part_index * heads_here, heads_here, 1)


def body(
    queries, new_keys, new_values, key_pool, value_pool, lengths, page_table, mig_slot, mig_dst
):
    replicas = lax.axis_size("rep")
    parts = lax.axis_size("tp")
    here_rep = lax.axis_index("rep")
    part_index = lax.axis_index("tp")
    slots, q_width = queries.shape
    k_width = new_keys.shape[1]
    heads_here = H // parts
    offset = mig_dst[0]
    start = (part_index * key_pool.shape[1]).reshape(1)
    visitor, keys_out, values_out = picked(
        page_table, mig_slot, queries, new_keys, new_values, key_pool, value_pool
    )

    def branch(distance):
        def run(visitor, keys_out, values_out):
            back = lax.ppermute(visitor, "rep", route_by(replicas, -distance))
            moved_keys = lax.ppermute(keys_out, "rep", route_by(replicas, distance))
            moved_values = lax.ppermute(values_out, "rep", route_by(replicas, distance))
            own_len = lax.dynamic_slice_in_dim(lengths, here_rep * slots, slots)
            tokens = jnp.concatenate([queries, new_keys, new_values], axis=1)
            tokens = tokens.reshape(slots, -1, DH)
            q_all, mine = shared(mig_slot, back, tokens, heads_here, parts)
            flat = mine[:, heads_here:].reshape(slots, 2 * k_width)
            token_keys = token_rows(flat[:, :k_width], parts, part_index)
            token_values = token_rows(flat[:, k_width:], parts, part_index)
            partials = attended_parts(
                page_table, own_len, start, q_all, key_pool, value_pool, parts
            )
            result, leaver = finished(mig_slot, partials, mine, token_keys, token_values)
            arrived = lax.ppermute(leaver, "rep", route_by(replicas, distance))
            return result, arrived, moved_keys, moved_values

        return run

    result, arrived, moved_keys, moved_values = lax.switch(
        offset - 1,
        [branch(distance) for distance in range(1, replicas)],
        visitor,
        keys_out,
        values_out,
    )
    return placed_results(mig_slot, result, arrived, moved_keys, moved_values)


def solution(mesh):
    placed = (
        P("rep", "tp"),
        P("rep", "tp"),
        P("rep", "tp"),
        P("rep", "tp", None),
        P("rep", "tp", None),
        P(),
        P("rep", None),
        P(),
        P(),
    )
    return jax.shard_map(
        body,
        mesh=mesh,
        in_specs=placed,
        out_specs=(P("rep", "tp"), P("rep", "tp", None), P("rep", "tp", None)),
        check_vma=False,
    )
```

```python
import math


import jax
import jax.numpy as jnp
from jax import lax
from jax.experimental import pallas as pl
from jax.experimental.pallas import tpu as pltpu
from jax.sharding import PartitionSpec as P

H = 64
KVH = 8
DH = 128
LOW = -1e30


def route_by(count, distance):
    return [(i, (i + distance) % count) for i in range(count)]


def pick_kernel(
    table_ref, mig_ref, q_ref, nk_ref, nv_ref, key_ref, value_ref, row_ref, kout_ref, vout_ref, sems
):
    pages = kout_ref.shape[0]
    leaving = mig_ref[lax.axis_index("rep")]

    @pl.loop(0, pages)
    def _(j):
        page = jnp.maximum(table_ref[leaving, j], 0)
        pltpu.make_async_copy(key_ref.at[page], kout_ref.at[j], sems.at[0]).start()
        pltpu.make_async_copy(value_ref.at[page], vout_ref.at[j], sems.at[1]).start()

    at = 0
    for ref in (q_ref, nk_ref, nv_ref):
        width = ref.shape[1]
        slot = lax.broadcasted_iota(jnp.int32, ref.shape, 0)
        chosen = jnp.where(slot == leaving, ref[...].astype(jnp.float32), 0.0)
        row = jnp.sum(chosen, axis=0, keepdims=True)
        row_ref[:, at : at + width] = row.astype(jnp.bfloat16)
        at += width
    pltpu.make_async_copy(key_ref.at[pl.ds(0, pages)], kout_ref, sems.at[0]).wait()
    pltpu.make_async_copy(value_ref.at[pl.ds(0, pages)], vout_ref, sems.at[1]).wait()

    @pl.loop(0, pages)
    def _(j):
        @pl.when(table_ref[leaving, j] < 0)
        def _():
            kout_ref[j] = jnp.zeros(kout_ref.shape[1:], kout_ref.dtype)
            vout_ref[j] = jnp.zeros(vout_ref.shape[1:], vout_ref.dtype)


def picked(table, mig_slot, queries, new_keys, new_values, key_pool, value_pool):
    shape = (table.shape[1],) + key_pool.shape[1:]
    width = queries.shape[1] + 2 * new_keys.shape[1]
    return pl.pallas_call(
        pick_kernel,
        out_shape=[
            jax.ShapeDtypeStruct((1, width), jnp.bfloat16),
            jax.ShapeDtypeStruct(shape, key_pool.dtype),
            jax.ShapeDtypeStruct(shape, key_pool.dtype),
        ],
        in_specs=[pl.BlockSpec(memory_space=pltpu.SMEM)] * 2
        + [pl.BlockSpec(memory_space=pltpu.VMEM)] * 3
        + [pl.BlockSpec(memory_space=pl.ANY)] * 2,
        out_specs=[pl.BlockSpec(memory_space=pltpu.VMEM)] * 3,
        scratch_shapes=[pltpu.SemaphoreType.DMA((2,))],
        compiler_params=pltpu.CompilerParams(vmem_limit_bytes=8 << 20),
        cost_estimate=pl.CostEstimate(
            flops=0, bytes_accessed=8 * math.prod(shape), transcendentals=0
        ),
    )(table, mig_slot, queries, new_keys, new_values, key_pool, value_pool)


def greet(parts):
    me = lax.axis_index("tp")
    barrier = pltpu.get_barrier_semaphore()
    for k in range(1, parts):
        pl.semaphore_signal(
            barrier,
            inc=1,
            device_id={"tp": lax.rem(me + k, parts)},
            device_id_type=pl.DeviceIdType.MESH,
        )
    pl.semaphore_wait(barrier, parts - 1)
    return me


def share_kernel(mig_ref, back_ref, tokens_ref, all_ref, mine_ref, own, send_sems, recv_sems):
    parts, slots, heads_here, _ = all_ref.shape
    chunks = tokens_ref.shape[1]
    leaving = mig_ref[lax.axis_index("rep")]
    back = back_ref[...].astype(jnp.float32)
    row = jnp.concatenate([back[:, h * DH : (h + 1) * DH] for h in range(chunks)], axis=0)
    for i in range(slots):
        value = jnp.where(leaving == i, row, tokens_ref[i].astype(jnp.float32))
        value = value.astype(jnp.bfloat16)
        mine_ref[i] = value
        own[i] = value[:heads_here]
    me = greet(parts)
    copies = []
    for k in range(1, parts):
        copy = pltpu.make_async_remote_copy(
            src_ref=own,
            dst_ref=all_ref.at[me],
            send_sem=send_sems.at[k - 1],
            recv_sem=recv_sems.at[k - 1],
            device_id={"tp": lax.rem(me + k, parts)},
            device_id_type=pl.DeviceIdType.MESH,
        )
        copy.start()
        copies.append(copy)
    all_ref[me] = own[...]
    for copy in copies:
        copy.wait()


def shared(mig_slot, back, tokens, heads_here, parts):
    slots = tokens.shape[0]
    return pl.pallas_call(
        share_kernel,
        out_shape=[
            jax.ShapeDtypeStruct((parts, slots, heads_here, DH), jnp.bfloat16),
            jax.ShapeDtypeStruct(tokens.shape, jnp.bfloat16),
        ],
        in_specs=[pl.BlockSpec(memory_space=pltpu.SMEM)]
        + [pl.BlockSpec(memory_space=pltpu.VMEM)] * 2,
        out_specs=[pl.BlockSpec(memory_space=pltpu.VMEM)] * 2,
        scratch_shapes=[
            pltpu.VMEM((slots, heads_here, DH), jnp.bfloat16),
            pltpu.SemaphoreType.DMA((parts - 1,)),
            pltpu.SemaphoreType.DMA((parts - 1,)),
        ],
        compiler_params=pltpu.CompilerParams(
            collective_id=0, has_side_effects=True, vmem_limit_bytes=8 << 20
        ),
        cost_estimate=pl.CostEstimate(flops=0, bytes_accessed=8 << 20, transcendentals=0),
    )(mig_slot, back, tokens)


def flat_rows(block):
    pages, rows, width = block.shape
    if rows % 16 == 0:
        return block.reshape(pages * rows, width)
    return block.astype(jnp.float32).reshape(pages * rows, width).astype(block.dtype)


def attend_kernel(
    table_ref,
    len_ref,
    start_ref,
    q_ref,
    key_ref,
    value_ref,
    out_ref,
    kbuf,
    vbuf,
    stats_ref,
    ksem,
    vsem,
):
    slots, pages, rows, width = kbuf.shape
    parts, heads_here = q_ref.shape[0], q_ref.shape[2]
    group = H // KVH
    page_len = rows * parts
    scaling = 1.0 / math.sqrt(DH)
    steps = 3 if pages % 3 == 0 else 1
    step_pages = pages // steps

    def live_pages(i):
        return lax.div(len_ref[i] + (page_len - 1), page_len)

    def key_copy(i, j):
        page = jnp.maximum(table_ref[i, j], 0)
        return pltpu.make_async_copy(key_ref.at[page], kbuf.at[i, j], ksem.at[i, j])

    def value_copy(i, j):
        page = jnp.maximum(table_ref[i, j], 0)
        return pltpu.make_async_copy(value_ref.at[page], vbuf.at[i, j], vsem.at[i, j])

    @pl.loop(0, slots)
    def _(i):
        @pl.loop(0, live_pages(i))
        def _(j):
            key_copy(i, j).start()
            value_copy(i, j).start()

    head = lax.broadcasted_iota(jnp.int32, (H, DH), 0) // group
    column = lax.broadcasted_iota(jnp.int32, (H, DH), 1)
    stats_ref[...] = jnp.zeros_like(stats_ref)

    def attend(i, used):
        tokens = used * rows
        lane = lax.broadcasted_iota(jnp.int32, (H, tokens), 1)
        position = (lane // rows) * page_len + lane % rows + start_ref[0]
        q = jnp.concatenate([q_ref[t, i].astype(jnp.float32) for t in range(parts)], axis=0)
        spread = jnp.concatenate(
            [jnp.where(head == g, q, 0.0).astype(jnp.bfloat16) for g in range(KVH)], axis=1
        )
        scores = lax.dot_general(
            spread,
            flat_rows(kbuf[i, 0:used]),
            (((1,), (1,)), ((), ())),
            preferred_element_type=jnp.float32,
        )
        usable = position < len_ref[i]
        masked = jnp.where(usable, scores * scaling, LOW)
        peak = jnp.max(masked, axis=1, keepdims=True)
        weights = jnp.where(usable, jnp.exp(masked - peak), 0.0)
        total = jnp.sum(weights, axis=1, keepdims=True)
        mixed = jnp.dot(
            weights.astype(jnp.bfloat16),
            flat_rows(vbuf[i, 0:used]),
            preferred_element_type=jnp.float32,
        )
        own = jnp.concatenate(
            [
                mixed[g * group : (g + 1) * group, g * DH : (g + 1) * DH]
                for g in range(KVH)
            ],
            axis=0,
        )
        for t in range(parts):
            out_ref[t, i] = own[t * heads_here : (t + 1) * heads_here]
        stats = jnp.where(column == i, peak, stats_ref[...])
        stats_ref[...] = jnp.where(column == i + slots, total, stats)

    @pl.loop(0, slots)
    def _(i):
        live = live_pages(i)
        needed = lax.div(live + (step_pages - 1), step_pages)

        @pl.loop(live, needed * step_pages)
        def _(j):
            vbuf[i, j] = jnp.zeros((rows, width), vbuf.dtype)

        @pl.loop(0, live)
        def _(j):
            key_copy(i, j).wait()
            value_copy(i, j).wait()

        for step in range(1, steps + 1):

            @pl.when(needed == step)
            def _():
                attend(i, step * step_pages)

    for t in range(parts):
        out_ref[t, slots] = stats_ref[t * heads_here : (t + 1) * heads_here]


def attended_parts(table, lens, start, q, key_pool, value_pool, parts):
    slots, pages = table.shape
    rows, width = key_pool.shape[1:]
    buffer = (slots, pages, rows, width)
    return pl.pallas_call(
        attend_kernel,
        out_shape=jax.ShapeDtypeStruct((parts, slots + 1, H // parts, DH), jnp.float32),
        in_specs=[pl.BlockSpec(memory_space=pltpu.SMEM)] * 3
        + [pl.BlockSpec(memory_space=pltpu.VMEM)]
        + [pl.BlockSpec(memory_space=pl.ANY)] * 2,
        out_specs=pl.BlockSpec(memory_space=pltpu.VMEM),
        scratch_shapes=[
            pltpu.VMEM(buffer, key_pool.dtype),
            pltpu.VMEM(buffer, value_pool.dtype),
            pltpu.VMEM((H, DH), jnp.float32),
            pltpu.SemaphoreType.DMA((slots, pages)),
            pltpu.SemaphoreType.DMA((slots, pages)),
        ],
        compiler_params=pltpu.CompilerParams(vmem_limit_bytes=24 << 20),
        cost_estimate=pl.CostEstimate(
            flops=4 * H * pages * rows * width * slots,
            bytes_accessed=4 * math.prod(buffer),
            transcendentals=0,
        ),
    )(table, lens, start, q, key_pool, value_pool)


def finish_kernel(
    mig_ref,
    part_ref,
    mine_ref,
    tk_ref,
    tv_ref,
    out_ref,
    leaver_ref,
    flat,
    landed,
    send_sems,
    recv_sems,
):
    parts, _, heads_here, _ = part_ref.shape
    slots = mine_ref.shape[0]
    repeat = heads_here // tk_ref.shape[1]
    leaving = mig_ref[lax.axis_index("rep")]
    scaling = 1.0 / math.sqrt(DH)
    me = greet(parts)
    copies = []
    for k in range(1, parts):
        peer = lax.rem(me + k, parts)
        copy = pltpu.make_async_remote_copy(
            src_ref=part_ref.at[peer],
            dst_ref=landed.at[k - 1],
            send_sem=send_sems.at[k - 1],
            recv_sem=recv_sems.at[k - 1],
            device_id={"tp": peer},
            device_id_type=pl.DeviceIdType.MESH,
        )
        copy.start()
        copies.append(copy)

    def spread(ref, i):
        value = ref[i].astype(jnp.float32)
        return jnp.concatenate(
            [
                jnp.broadcast_to(value[g : g + 1], (repeat, DH))
                for g in range(value.shape[0])
            ],
            axis=0,
        )

    fresh, values = [], []
    for i in range(slots):
        q = mine_ref[i].astype(jnp.float32)[:heads_here]
        fresh.append(jnp.sum(q * spread(tk_ref, i), axis=-1, keepdims=True) * scaling)
        values.append(spread(tv_ref, i))
    for copy in copies:
        copy.wait()
    stats = [part_ref[me, slots]] + [landed[k, slots] for k in range(parts - 1)]
    leaver = jnp.zeros((heads_here, DH), jnp.float32)
    for i in range(slots):
        top = fresh[i]
        for stat in stats:
            top = jnp.maximum(top, stat[:, i : i + 1])
        weight = jnp.exp(fresh[i] - top)
        total = weight
        mixed = weight.astype(jnp.bfloat16).astype(jnp.float32) * values[i]
        for k, stat in enumerate(stats):
            scale = jnp.exp(stat[:, i : i + 1] - top)
            block = part_ref[me, i] if k == 0 else landed[k - 1, i]
            total = total + scale * stat[:, slots + i : slots + i + 1]
            mixed = mixed + scale * block
        result = mixed / total
        leaver = jnp.where(leaving == i, result, leaver)
        for h in range(heads_here):
            flat[i : i + 1, h * DH : (h + 1) * DH] = result[h : h + 1]
    out_ref[...] = flat[...].astype(out_ref.dtype)
    row = jnp.concatenate([leaver[h : h + 1] for h in range(heads_here)], axis=1)
    leaver_ref[...] = row.astype(leaver_ref.dtype)


def finished(mig_slot, partials, mine, token_keys, token_values):
    parts, _, heads_here, _ = partials.shape
    slots = mine.shape[0]
    return pl.pallas_call(
        finish_kernel,
        out_shape=[
            jax.ShapeDtypeStruct((slots, heads_here * DH), jnp.bfloat16),
            jax.ShapeDtypeStruct((1, heads_here * DH), jnp.bfloat16),
        ],
        in_specs=[pl.BlockSpec(memory_space=pltpu.SMEM)]
        + [pl.BlockSpec(memory_space=pltpu.VMEM)] * 4,
        out_specs=[pl.BlockSpec(memory_space=pltpu.VMEM)] * 2,
        scratch_shapes=[
            pltpu.VMEM((slots, heads_here * DH), jnp.float32),
            pltpu.VMEM((parts - 1,) + partials.shape[1:], jnp.float32),
            pltpu.SemaphoreType.DMA((parts - 1,)),
            pltpu.SemaphoreType.DMA((parts - 1,)),
        ],
        compiler_params=pltpu.CompilerParams(
            collective_id=1, has_side_effects=True, vmem_limit_bytes=8 << 20
        ),
        cost_estimate=pl.CostEstimate(flops=0, bytes_accessed=8 << 20, transcendentals=0),
    )(mig_slot, partials, mine, token_keys, token_values)


def place_kernel(
    mig_ref, result_ref, row_ref, key_ref, value_ref, out_ref, kout_ref, vout_ref, kbuf, vbuf, sems
):
    pages = kbuf.shape[0]
    lanes = ((key_ref, kbuf, kout_ref), (value_ref, vbuf, vout_ref))
    span = 3 if pages % 3 == 0 else 1
    cuts = [pl.ds(j, span) for j in range(0, pages, span)]
    pairs = [(n, c) for c in range(len(cuts)) for n in range(2)]
    for n, c in pairs:
        source, buf, _ = lanes[n]
        pltpu.make_async_copy(source.at[cuts[c]], buf.at[cuts[c]], sems.at[n, c]).start()
    leaving = mig_ref[lax.axis_index("rep")]
    slot = lax.broadcasted_iota(jnp.int32, result_ref.shape, 0)
    row = row_ref[...].astype(jnp.float32)
    result = result_ref[...].astype(jnp.float32)
    out_ref[...] = jnp.where(slot == leaving, row, result).astype(out_ref.dtype)
    for n, c in pairs:
        source, buf, sink = lanes[n]
        pltpu.make_async_copy(source.at[cuts[c]], buf.at[cuts[c]], sems.at[n, c]).wait()
        pltpu.make_async_copy(buf.at[cuts[c]], sink.at[cuts[c]], sems.at[n, c]).start()
    for n, c in pairs:
        _, buf, sink = lanes[n]
        pltpu.make_async_copy(buf.at[cuts[c]], sink.at[cuts[c]], sems.at[n, c]).wait()


def placed_results(mig_slot, result, row, moved_keys, moved_values):
    moved = jax.ShapeDtypeStruct(moved_keys.shape, moved_keys.dtype)
    return pl.pallas_call(
        place_kernel,
        out_shape=[jax.ShapeDtypeStruct(result.shape, result.dtype), moved, moved],
        in_specs=[pl.BlockSpec(memory_space=pltpu.SMEM)]
        + [pl.BlockSpec(memory_space=pltpu.VMEM)] * 2
        + [pl.BlockSpec(memory_space=pl.ANY)] * 2,
        out_specs=[pl.BlockSpec(memory_space=pltpu.VMEM)]
        + [pl.BlockSpec(memory_space=pl.ANY)] * 2,
        scratch_shapes=[
            pltpu.VMEM(moved.shape, moved.dtype),
            pltpu.VMEM(moved.shape, moved.dtype),
            pltpu.SemaphoreType.DMA((2, moved.shape[0])),
        ],
        compiler_params=pltpu.CompilerParams(vmem_limit_bytes=8 << 20),
    )(mig_slot, result, row, moved_keys, moved_values)


def token_rows(fresh, parts, part_index):
    slots, width = fresh.shape
    heads_here = H // parts
    if width % DH == 0:
        return fresh.reshape(slots, width // DH, DH)
    every = lax.all_gather(fresh, "tp", axis=1, tiled=True).reshape(slots, KVH, DH)
    every = jnp.repeat(every, H // KVH, axis=1)
    return lax.dynamic_slice_in_dim(every, part_index * heads_here, heads_here, 1)


def body(
    queries, new_keys, new_values, key_pool, value_pool, lengths, page_table, mig_slot, mig_dst
):
    replicas = lax.axis_size("rep")
    parts = lax.axis_size("tp")
    here_rep = lax.axis_index("rep")
    part_index = lax.axis_index("tp")
    slots, _ = queries.shape
    k_width = new_keys.shape[1]
    heads_here = H // parts
    offset = mig_dst[0]
    start = (part_index * key_pool.shape[1]).reshape(1)
    visitor, keys_out, values_out = picked(
        page_table, mig_slot, queries, new_keys, new_values, key_pool, value_pool
    )

    def branch(distance):
        def run(visitor, keys_out, values_out):
            back = lax.ppermute(visitor, "rep", route_by(replicas, -distance))
            moved_keys = lax.ppermute(keys_out, "rep", route_by(replicas, distance))
            moved_values = lax.ppermute(values_out, "rep", route_by(replicas, distance))
            own_len = lax.dynamic_slice_in_dim(lengths, here_rep * slots, slots)
            tokens = jnp.concatenate([queries, new_keys, new_values], axis=1)
            tokens = tokens.reshape(slots, -1, DH)
            q_all, mine = shared(mig_slot, back, tokens, heads_here, parts)
            flat = mine[:, heads_here:].reshape(slots, 2 * k_width)
            token_keys = token_rows(flat[:, :k_width], parts, part_index)
            token_values = token_rows(flat[:, k_width:], parts, part_index)
            partials = attended_parts(
                page_table, own_len, start, q_all, key_pool, value_pool, parts
            )
            result, leaver = finished(mig_slot, partials, mine, token_keys, token_values)
            arrived = lax.ppermute(leaver, "rep", route_by(replicas, distance))
            return result, arrived, moved_keys, moved_values

        return run

    result, arrived, moved_keys, moved_values = lax.switch(
        offset - 1,
        [branch(distance) for distance in range(1, replicas)],
        visitor,
        keys_out,
        values_out,
    )
    return placed_results(mig_slot, result, arrived, moved_keys, moved_values)


def solution(mesh):
    placed = (
        P("rep", "tp"),
        P("rep", "tp"),
        P("rep", "tp"),
        P("rep", "tp", None),
        P("rep", "tp", None),
        P(),
        P("rep", None),
        P(),
        P(),
    )
    return jax.shard_map(
        body,
        mesh=mesh,
        in_specs=placed,
        out_specs=(P("rep", "tp"), P("rep", "tp", None), P("rep", "tp", None)),
        check_vma=False,
    )
```

```python
import math


import jax
import jax.numpy as jnp
from jax import lax
from jax.experimental import pallas as pl
from jax.experimental.pallas import tpu as pltpu
from jax.sharding import PartitionSpec as P

H = 64
KVH = 8
DH = 128
LOW = -1e30


def route_by(count, distance):
    return [(i, (i + distance) % count) for i in range(count)]


def pick_kernel(
    table_ref,
    mig_ref,
    q_ref,
    nk_ref,
    nv_ref,
    key_ref,
    value_ref,
    row_ref,
    kout_ref,
    vout_ref,
    q_buf,
    nk_buf,
    nv_buf,
    sems,
    row_sems,
):
    fills = ((q_ref, q_buf), (nk_ref, nk_buf), (nv_ref, nv_buf))
    for n, (ref, buf) in enumerate(fills):
        pltpu.make_async_copy(ref, buf, row_sems.at[n]).start()
    pages = kout_ref.shape[0]
    leaving = mig_ref[lax.axis_index("rep")]

    @pl.loop(0, pages)
    def _(j):
        page = jnp.maximum(table_ref[leaving, j], 0)
        pltpu.make_async_copy(key_ref.at[page], kout_ref.at[j], sems.at[0]).start()
        pltpu.make_async_copy(value_ref.at[page], vout_ref.at[j], sems.at[1]).start()

    at = 0
    for n, (ref, buf) in enumerate(fills):
        pltpu.make_async_copy(ref, buf, row_sems.at[n]).wait()
        width = buf.shape[1]
        slot = lax.broadcasted_iota(jnp.int32, buf.shape, 0)
        chosen = jnp.where(slot == leaving, buf[...].astype(jnp.float32), 0.0)
        row = jnp.sum(chosen, axis=0, keepdims=True)
        row_ref[:, at : at + width] = row.astype(jnp.bfloat16)
        at += width
    pltpu.make_async_copy(key_ref.at[pl.ds(0, pages)], kout_ref, sems.at[0]).wait()
    pltpu.make_async_copy(value_ref.at[pl.ds(0, pages)], vout_ref, sems.at[1]).wait()

    @pl.loop(0, pages)
    def _(j):
        @pl.when(table_ref[leaving, j] < 0)
        def _():
            kout_ref[j] = jnp.zeros(kout_ref.shape[1:], kout_ref.dtype)
            vout_ref[j] = jnp.zeros(vout_ref.shape[1:], vout_ref.dtype)


def picked(table, mig_slot, queries, new_keys, new_values, key_pool, value_pool):
    shape = (table.shape[1],) + key_pool.shape[1:]
    width = queries.shape[1] + 2 * new_keys.shape[1]
    return pl.pallas_call(
        pick_kernel,
        out_shape=[
            jax.ShapeDtypeStruct((1, width), jnp.bfloat16),
            jax.ShapeDtypeStruct(shape, key_pool.dtype),
            jax.ShapeDtypeStruct(shape, key_pool.dtype),
        ],
        in_specs=[pl.BlockSpec(memory_space=pltpu.SMEM)] * 2
        + [pl.BlockSpec(memory_space=pl.ANY)] * 5,
        out_specs=[pl.BlockSpec(memory_space=pltpu.VMEM)] * 3,
        scratch_shapes=[
            pltpu.VMEM(queries.shape, queries.dtype),
            pltpu.VMEM(new_keys.shape, new_keys.dtype),
            pltpu.VMEM(new_values.shape, new_values.dtype),
            pltpu.SemaphoreType.DMA((2,)),
            pltpu.SemaphoreType.DMA((3,)),
        ],
        compiler_params=pltpu.CompilerParams(vmem_limit_bytes=8 << 20),
        cost_estimate=pl.CostEstimate(
            flops=0, bytes_accessed=8 * math.prod(shape), transcendentals=0
        ),
    )(table, mig_slot, queries, new_keys, new_values, key_pool, value_pool)


def greet(parts):
    me = lax.axis_index("tp")
    barrier = pltpu.get_barrier_semaphore()
    for k in range(1, parts):
        pl.semaphore_signal(
            barrier,
            inc=1,
            device_id={"tp": lax.rem(me + k, parts)},
            device_id_type=pl.DeviceIdType.MESH,
        )
    pl.semaphore_wait(barrier, parts - 1)
    return me


def share_kernel(mig_ref, back_ref, tokens_ref, all_ref, mine_ref, own, send_sems, recv_sems):
    parts, slots, heads_here, _ = all_ref.shape
    chunks = tokens_ref.shape[1]
    leaving = mig_ref[lax.axis_index("rep")]
    back = back_ref[...].astype(jnp.float32)
    row = jnp.concatenate([back[:, h * DH : (h + 1) * DH] for h in range(chunks)], axis=0)
    for i in range(slots):
        value = jnp.where(leaving == i, row, tokens_ref[i].astype(jnp.float32))
        value = value.astype(jnp.bfloat16)
        mine_ref[i] = value
        own[i] = value[:heads_here]
    me = greet(parts)
    copies = []
    for k in range(1, parts):
        copy = pltpu.make_async_remote_copy(
            src_ref=own,
            dst_ref=all_ref.at[me],
            send_sem=send_sems.at[k - 1],
            recv_sem=recv_sems.at[k - 1],
            device_id={"tp": lax.rem(me + k, parts)},
            device_id_type=pl.DeviceIdType.MESH,
        )
        copy.start()
        copies.append(copy)
    all_ref[me] = own[...]
    for copy in copies:
        copy.wait()


def shared(mig_slot, back, tokens, heads_here, parts):
    slots = tokens.shape[0]
    return pl.pallas_call(
        share_kernel,
        out_shape=[
            jax.ShapeDtypeStruct((parts, slots, heads_here, DH), jnp.bfloat16),
            jax.ShapeDtypeStruct(tokens.shape, jnp.bfloat16),
        ],
        in_specs=[pl.BlockSpec(memory_space=pltpu.SMEM)]
        + [pl.BlockSpec(memory_space=pltpu.VMEM)] * 2,
        out_specs=[pl.BlockSpec(memory_space=pltpu.VMEM)] * 2,
        scratch_shapes=[
            pltpu.VMEM((slots, heads_here, DH), jnp.bfloat16),
            pltpu.SemaphoreType.DMA((parts - 1,)),
            pltpu.SemaphoreType.DMA((parts - 1,)),
        ],
        compiler_params=pltpu.CompilerParams(
            collective_id=0, has_side_effects=True, vmem_limit_bytes=8 << 20
        ),
        cost_estimate=pl.CostEstimate(flops=0, bytes_accessed=8 << 20, transcendentals=0),
    )(mig_slot, back, tokens)


def flat_rows(block):
    pages, rows, width = block.shape
    if rows % 16 == 0:
        return block.reshape(pages * rows, width)
    return block.astype(jnp.float32).reshape(pages * rows, width).astype(block.dtype)


def attend_kernel(
    table_ref,
    len_ref,
    start_ref,
    q_ref,
    key_ref,
    value_ref,
    out_ref,
    kbuf,
    vbuf,
    stats_ref,
    ksem,
    vsem,
):
    slots, pages, rows, width = kbuf.shape
    parts, heads_here = q_ref.shape[0], q_ref.shape[2]
    group = H // KVH
    page_len = rows * parts
    scaling = 1.0 / math.sqrt(DH)
    steps = 3 if pages % 3 == 0 else 1
    step_pages = pages // steps

    def live_pages(i):
        return lax.div(len_ref[i] + (page_len - 1), page_len)

    def key_copy(i, j):
        page = jnp.maximum(table_ref[i, j], 0)
        return pltpu.make_async_copy(key_ref.at[page], kbuf.at[i, j], ksem.at[i, j])

    def value_copy(i, j):
        page = jnp.maximum(table_ref[i, j], 0)
        return pltpu.make_async_copy(value_ref.at[page], vbuf.at[i, j], vsem.at[i, j])

    @pl.loop(0, slots)
    def _(i):
        @pl.loop(0, live_pages(i))
        def _(j):
            key_copy(i, j).start()
            value_copy(i, j).start()

    head = lax.broadcasted_iota(jnp.int32, (H, DH), 0) // group
    column = lax.broadcasted_iota(jnp.int32, (H, DH), 1)
    stats_ref[...] = jnp.zeros_like(stats_ref)

    def attend(i, used):
        tokens = used * rows
        lane = lax.broadcasted_iota(jnp.int32, (H, tokens), 1)
        position = (lane // rows) * page_len + lane % rows + start_ref[0]
        q = jnp.concatenate([q_ref[t, i].astype(jnp.float32) for t in range(parts)], axis=0)
        spread = jnp.concatenate(
            [jnp.where(head == g, q, 0.0).astype(jnp.bfloat16) for g in range(KVH)], axis=1
        )
        scores = lax.dot_general(
            spread,
            flat_rows(kbuf[i, 0:used]),
            (((1,), (1,)), ((), ())),
            preferred_element_type=jnp.float32,
        )
        usable = position < len_ref[i]
        masked = jnp.where(usable, scores * scaling, LOW)
        peak = jnp.max(masked, axis=1, keepdims=True)
        weights = jnp.where(usable, jnp.exp(masked - peak), 0.0)
        total = jnp.sum(weights, axis=1, keepdims=True)
        mixed = jnp.dot(
            weights.astype(jnp.bfloat16),
            flat_rows(vbuf[i, 0:used]),
            preferred_element_type=jnp.float32,
        )
        own = jnp.concatenate(
            [
                mixed[g * group : (g + 1) * group, g * DH : (g + 1) * DH]
                for g in range(KVH)
            ],
            axis=0,
        )
        for t in range(parts):
            out_ref[t, i] = own[t * heads_here : (t + 1) * heads_here]
        stats = jnp.where(column == i, peak, stats_ref[...])
        stats_ref[...] = jnp.where(column == i + slots, total, stats)

    @pl.loop(0, slots)
    def _(i):
        live = live_pages(i)
        needed = lax.div(live + (step_pages - 1), step_pages)

        @pl.loop(live, needed * step_pages)
        def _(j):
            vbuf[i, j] = jnp.zeros((rows, width), vbuf.dtype)

        @pl.loop(0, live)
        def _(j):
            key_copy(i, j).wait()
            value_copy(i, j).wait()

        for step in range(1, steps + 1):

            @pl.when(needed == step)
            def _():
                attend(i, step * step_pages)

    for t in range(parts):
        out_ref[t, slots] = stats_ref[t * heads_here : (t + 1) * heads_here]


def attended_parts(table, lens, start, q, key_pool, value_pool, parts):
    slots, pages = table.shape
    rows, width = key_pool.shape[1:]
    buffer = (slots, pages, rows, width)
    return pl.pallas_call(
        attend_kernel,
        out_shape=jax.ShapeDtypeStruct((parts, slots + 1, H // parts, DH), jnp.float32),
        in_specs=[pl.BlockSpec(memory_space=pltpu.SMEM)] * 3
        + [pl.BlockSpec(memory_space=pltpu.VMEM)]
        + [pl.BlockSpec(memory_space=pl.ANY)] * 2,
        out_specs=pl.BlockSpec(memory_space=pltpu.VMEM),
        scratch_shapes=[
            pltpu.VMEM(buffer, key_pool.dtype),
            pltpu.VMEM(buffer, value_pool.dtype),
            pltpu.VMEM((H, DH), jnp.float32),
            pltpu.SemaphoreType.DMA((slots, pages)),
            pltpu.SemaphoreType.DMA((slots, pages)),
        ],
        compiler_params=pltpu.CompilerParams(vmem_limit_bytes=24 << 20),
        cost_estimate=pl.CostEstimate(
            flops=4 * H * pages * rows * width * slots,
            bytes_accessed=4 * math.prod(buffer),
            transcendentals=0,
        ),
    )(table, lens, start, q, key_pool, value_pool)


def finish_kernel(
    mig_ref,
    part_ref,
    mine_ref,
    tk_ref,
    tv_ref,
    out_ref,
    leaver_ref,
    flat,
    landed,
    send_sems,
    recv_sems,
):
    parts, _, heads_here, _ = part_ref.shape
    slots = mine_ref.shape[0]
    repeat = heads_here // tk_ref.shape[1]
    leaving = mig_ref[lax.axis_index("rep")]
    scaling = 1.0 / math.sqrt(DH)
    me = greet(parts)
    copies = []
    for k in range(1, parts):
        peer = lax.rem(me + k, parts)
        copy = pltpu.make_async_remote_copy(
            src_ref=part_ref.at[peer],
            dst_ref=landed.at[k - 1],
            send_sem=send_sems.at[k - 1],
            recv_sem=recv_sems.at[k - 1],
            device_id={"tp": peer},
            device_id_type=pl.DeviceIdType.MESH,
        )
        copy.start()
        copies.append(copy)

    def spread(ref, i):
        value = ref[i].astype(jnp.float32)
        return jnp.concatenate(
            [
                jnp.broadcast_to(value[g : g + 1], (repeat, DH))
                for g in range(value.shape[0])
            ],
            axis=0,
        )

    fresh, values = [], []
    for i in range(slots):
        q = mine_ref[i].astype(jnp.float32)[:heads_here]
        fresh.append(jnp.sum(q * spread(tk_ref, i), axis=-1, keepdims=True) * scaling)
        values.append(spread(tv_ref, i))
    for copy in copies:
        copy.wait()
    stats = [part_ref[me, slots]] + [landed[k, slots] for k in range(parts - 1)]
    leaver = jnp.zeros((heads_here, DH), jnp.float32)
    for i in range(slots):
        top = fresh[i]
        for stat in stats:
            top = jnp.maximum(top, stat[:, i : i + 1])
        weight = jnp.exp(fresh[i] - top)
        total = weight
        mixed = weight.astype(jnp.bfloat16).astype(jnp.float32) * values[i]
        for k, stat in enumerate(stats):
            scale = jnp.exp(stat[:, i : i + 1] - top)
            block = part_ref[me, i] if k == 0 else landed[k - 1, i]
            total = total + scale * stat[:, slots + i : slots + i + 1]
            mixed = mixed + scale * block
        result = mixed / total
        leaver = jnp.where(leaving == i, result, leaver)
        for h in range(heads_here):
            flat[i : i + 1, h * DH : (h + 1) * DH] = result[h : h + 1]
    out_ref[...] = flat[...].astype(out_ref.dtype)
    row = jnp.concatenate([leaver[h : h + 1] for h in range(heads_here)], axis=1)
    leaver_ref[...] = row.astype(leaver_ref.dtype)


def finished(mig_slot, partials, mine, token_keys, token_values):
    parts, _, heads_here, _ = partials.shape
    slots = mine.shape[0]
    return pl.pallas_call(
        finish_kernel,
        out_shape=[
            jax.ShapeDtypeStruct((slots, heads_here * DH), jnp.bfloat16),
            jax.ShapeDtypeStruct((1, heads_here * DH), jnp.bfloat16),
        ],
        in_specs=[pl.BlockSpec(memory_space=pltpu.SMEM)]
        + [pl.BlockSpec(memory_space=pltpu.VMEM)] * 4,
        out_specs=[pl.BlockSpec(memory_space=pltpu.VMEM)] * 2,
        scratch_shapes=[
            pltpu.VMEM((slots, heads_here * DH), jnp.float32),
            pltpu.VMEM((parts - 1,) + partials.shape[1:], jnp.float32),
            pltpu.SemaphoreType.DMA((parts - 1,)),
            pltpu.SemaphoreType.DMA((parts - 1,)),
        ],
        compiler_params=pltpu.CompilerParams(
            collective_id=1, has_side_effects=True, vmem_limit_bytes=8 << 20
        ),
        cost_estimate=pl.CostEstimate(flops=0, bytes_accessed=8 << 20, transcendentals=0),
    )(mig_slot, partials, mine, token_keys, token_values)


def place_kernel(
    mig_ref,
    result_ref,
    row_ref,
    key_ref,
    value_ref,
    out_ref,
    kout_ref,
    vout_ref,
    kbuf,
    vbuf,
    rowbuf,
    outbuf,
    sems,
    row_sem,
    out_sem,
):
    pages = kbuf.shape[0]
    pltpu.make_async_copy(row_ref, rowbuf, row_sem).start()
    lanes = ((key_ref, kbuf, kout_ref), (value_ref, vbuf, vout_ref))
    span = 3 if pages % 3 == 0 else 1
    cuts = [pl.ds(j, span) for j in range(0, pages, span)]
    pairs = [(n, c) for c in range(len(cuts)) for n in range(2)]
    for n, c in pairs:
        source, buf, _ = lanes[n]
        pltpu.make_async_copy(source.at[cuts[c]], buf.at[cuts[c]], sems.at[n, c]).start()
    leaving = mig_ref[lax.axis_index("rep")]
    slot = lax.broadcasted_iota(jnp.int32, result_ref.shape, 0)
    pltpu.make_async_copy(row_ref, rowbuf, row_sem).wait()
    row = rowbuf[...].astype(jnp.float32)
    result = result_ref[...].astype(jnp.float32)
    outbuf[...] = jnp.where(slot == leaving, row, result).astype(outbuf.dtype)
    for n, c in pairs:
        source, buf, sink = lanes[n]
        pltpu.make_async_copy(source.at[cuts[c]], buf.at[cuts[c]], sems.at[n, c]).wait()
        pltpu.make_async_copy(buf.at[cuts[c]], sink.at[cuts[c]], sems.at[n, c]).start()
    pltpu.make_async_copy(outbuf, out_ref, out_sem).start()
    for n, c in pairs:
        _, buf, sink = lanes[n]
        pltpu.make_async_copy(buf.at[cuts[c]], sink.at[cuts[c]], sems.at[n, c]).wait()
    pltpu.make_async_copy(outbuf, out_ref, out_sem).wait()


def placed_results(mig_slot, result, row, moved_keys, moved_values):
    moved = jax.ShapeDtypeStruct(moved_keys.shape, moved_keys.dtype)
    return pl.pallas_call(
        place_kernel,
        out_shape=[jax.ShapeDtypeStruct(result.shape, result.dtype), moved, moved],
        in_specs=[pl.BlockSpec(memory_space=pltpu.SMEM)]
        + [pl.BlockSpec(memory_space=pltpu.VMEM)]
        + [pl.BlockSpec(memory_space=pl.ANY)] * 3,
        out_specs=[pl.BlockSpec(memory_space=pl.ANY)] * 3,
        scratch_shapes=[
            pltpu.VMEM(moved.shape, moved.dtype),
            pltpu.VMEM(moved.shape, moved.dtype),
            pltpu.VMEM(row.shape, row.dtype),
            pltpu.VMEM(result.shape, result.dtype),
            pltpu.SemaphoreType.DMA((2, moved.shape[0])),
            pltpu.SemaphoreType.DMA,
            pltpu.SemaphoreType.DMA,
        ],
        compiler_params=pltpu.CompilerParams(vmem_limit_bytes=8 << 20),
    )(mig_slot, result, row, moved_keys, moved_values)


def token_rows(fresh, parts, part_index):
    slots, width = fresh.shape
    heads_here = H // parts
    if width % DH == 0:
        return fresh.reshape(slots, width // DH, DH)
    every = lax.all_gather(fresh, "tp", axis=1, tiled=True).reshape(slots, KVH, DH)
    every = jnp.repeat(every, H // KVH, axis=1)
    return lax.dynamic_slice_in_dim(every, part_index * heads_here, heads_here, 1)


def body(
    queries, new_keys, new_values, key_pool, value_pool, lengths, page_table, mig_slot, mig_dst
):
    replicas = lax.axis_size("rep")
    parts = lax.axis_size("tp")
    here_rep = lax.axis_index("rep")
    part_index = lax.axis_index("tp")
    slots, _ = queries.shape
    k_width = new_keys.shape[1]
    heads_here = H // parts
    offset = mig_dst[0]
    start = (part_index * key_pool.shape[1]).reshape(1)
    visitor, keys_out, values_out = picked(
        page_table, mig_slot, queries, new_keys, new_values, key_pool, value_pool
    )

    def branch(distance):
        def run(visitor, keys_out, values_out):
            back = lax.ppermute(visitor, "rep", route_by(replicas, -distance))
            moved_keys = lax.ppermute(keys_out, "rep", route_by(replicas, distance))
            moved_values = lax.ppermute(values_out, "rep", route_by(replicas, distance))
            own_len = lax.dynamic_slice_in_dim(lengths, here_rep * slots, slots)
            tokens = jnp.concatenate([queries, new_keys, new_values], axis=1)
            tokens = tokens.reshape(slots, -1, DH)
            q_all, mine = shared(mig_slot, back, tokens, heads_here, parts)
            flat = mine[:, heads_here:].reshape(slots, 2 * k_width)
            token_keys = token_rows(flat[:, :k_width], parts, part_index)
            token_values = token_rows(flat[:, k_width:], parts, part_index)
            partials = attended_parts(
                page_table, own_len, start, q_all, key_pool, value_pool, parts
            )
            result, leaver = finished(mig_slot, partials, mine, token_keys, token_values)
            arrived = lax.ppermute(leaver, "rep", route_by(replicas, distance))
            return result, arrived, moved_keys, moved_values

        return run

    result, arrived, moved_keys, moved_values = lax.switch(
        offset - 1,
        [branch(distance) for distance in range(1, replicas)],
        visitor,
        keys_out,
        values_out,
    )
    return placed_results(mig_slot, result, arrived, moved_keys, moved_values)


def solution(mesh):
    placed = (
        P("rep", "tp"),
        P("rep", "tp"),
        P("rep", "tp"),
        P("rep", "tp", None),
        P("rep", "tp", None),
        P(),
        P("rep", None),
        P(),
        P(),
    )
    return jax.shard_map(
        body,
        mesh=mesh,
        in_specs=placed,
        out_specs=(P("rep", "tp"), P("rep", "tp", None), P("rep", "tp", None)),
        check_vma=False,
    )
```
